32 devices in a mesh: ma: 16 (over z, y, core), freq: 2 (over x).
Axes of the slice: x: 2, y: 2, z: 4, core: 2. Of those that a mesh axis runs over, the one named last changes fastest.
Arguments:
- right_side: float32 [128, 8, 2, 512], P('ma', 'freq'), may hold values from -60 to 60
- start_field: float32 [128, 8, 2, 512], P('ma', 'freq'), may hold values from -6 to 6
- beam: float32 [128, 8, 2, 16, 512], P('ma', 'freq'), may hold values from -0.75 to 0.75
- noise: float32 [128, 8, 16], P('ma', 'freq'), may hold values from 0.3 to 3
- inv_power: float32 [512], replicated, may hold values from 0.5 to 2
- smooth: float32 [512], replicated, may hold values from 0.5 to 4
Outputs:
- solution_field: float32 [128, 8, 2, 512], P('ma', 'freq')
- residual: float32 [128, 8, 2, 512], P('ma', 'freq')
The draws below stay inside these ranges and needn't reach their ends.
All inputs are finite; a program needn't handle non-finite values.
Results may differ from the reference program's by a relative error of at most 0.0003.
Values sent between devices are 32-bit elements; how exact they have to be, the bound alone decides.
No kernel may reach another device: no remote copies, remote signals or barrier semaphores. Data moves between devices by JAX's collectives and lax.ppermute only.
A program may use at most 64 MiB of HBM per device.

```python
import math
import jax
import jax.numpy as jnp
from jax import lax

ELL = 512
RANK = 16
ITERS = 2
M = 128
FREQ = 8


def draw_right_side(key, part):
    key_values = jax.random.fold_in(key, 0)
    position = jnp.arange(M, dtype=jnp.float32) / M
    row_scale = jnp.power(10.0, position)
    values = jnp.clip(jax.random.normal(key_values, (M, FREQ, 2, ELL), jnp.float32), -6.0, 6.0)
    return jnp.clip(values * row_scale[:, None, None, None], -60.0, 60.0)


def block_scale(own_key, dims, pieces, low, largest):
    loudness, own = 1.0, jax.random.fold_in(own_key, 6)
    for axis_at, shards_of in pieces:
        draws = jnp.exp(jax.random.uniform(jax.random.fold_in(own, axis_at), (shards_of,), jnp.float32, low / len(pieces), largest / len(pieces)))
        loudness = loudness * jnp.repeat(draws, dims[axis_at] // shards_of).reshape([-1 if axis == axis_at else 1 for axis in range(len(dims))])
    return loudness


def gaussian(own_key, dims, spread, reach, cuts=(), held_as=jnp.bfloat16):
    drawn = spread * jax.random.normal(own_key, dims, jnp.float32)
    if cuts:
        drawn = drawn * block_scale(own_key, dims, cuts, -0.22, 0.18)
    return jnp.clip(drawn, -reach, reach).astype(held_as)


def setup_inputs(seed: int = 0) -> dict:
    splits = jax.random.split(jax.random.key(seed), 7)
    return {
        "right_side": draw_right_side(jax.random.fold_in(splits[6], 71), 0),
        "start_field": gaussian(splits[1], (M, FREQ, 2, ELL), 1.0, 6.0, ((0, 16), (1, 2)), jnp.float32),
        "beam": gaussian(splits[2], (M, FREQ, 2, RANK, ELL), (4 * RANK) ** -0.5, 0.75, ((0, 16), (1, 2)), jnp.float32),
        "noise": jnp.clip(jnp.exp(math.log(3.0) - 2.3025851 * jax.random.uniform(splits[3], (M, FREQ, RANK), jnp.float32) ** block_scale(splits[3], (M, FREQ, RANK), ((0, 16), (1, 2)), -0.2, 0.2)), 0.3, 3.0),
        "inv_power": jnp.clip(jnp.exp(jax.random.uniform(splits[4], (ELL,), jnp.float32, math.log(0.5), math.log(2.0))), 0.5, 2.0),
        "smooth": jnp.clip(jnp.exp(jax.random.uniform(splits[5], (ELL,), jnp.float32, math.log(0.5), math.log(4.0))), 0.5, 4.0),
    }


def beam_image(field, beam, noise):
    projected = jnp.einsum('mfakl,mfbl->mfabk', beam, field, precision=lax.Precision.HIGHEST)
    real_part = projected[:, :, 0, 0] + projected[:, :, 1, 1]
    imaginary = projected[:, :, 0, 1] - projected[:, :, 1, 0]
    weighted = jnp.stack([real_part, imaginary], axis=2) * noise[:, :, None, :]
    back = jnp.einsum('mfakl,mfbk->mfabl', beam, weighted, precision=lax.Precision.HIGHEST)
    return jnp.stack([back[:, :, 0, 0] - back[:, :, 1, 1], back[:, :, 0, 1] + back[:, :, 1, 0]], axis=2)


def operate(field, beam, noise, inv_power, smooth):
    padded = jnp.pad(field, ((0, 0), (1, 1), (0, 0), (0, 0)))
    channel = jnp.arange(field.shape[1], dtype=jnp.int32)
    weight = (channel > 0).astype(jnp.float32) + (channel < field.shape[1] - 1).astype(jnp.float32)
    prior = smooth * (weight[None, :, None, None] * field - padded[:, :-2] - padded[:, 2:])
    return beam_image(field, beam, noise) + inv_power * field + prior


def reference(right_side, start_field, beam, noise, inv_power, smooth):
    solution_field = start_field
    resid_now = right_side - operate(start_field, beam, noise, inv_power, smooth)
    direction = resid_now
    norm_now = jnp.sum(resid_now * resid_now)
    for turn in range(ITERS):
        applied = operate(direction, beam, noise, inv_power, smooth)
        step_size = norm_now / jnp.sum(direction * applied)
        solution_field = solution_field + step_size * direction
        resid_now = resid_now - step_size * applied
        norm_next = jnp.sum(resid_now * resid_now)
        direction = resid_now + (norm_next / norm_now) * direction
        norm_now = norm_next
    return solution_field, resid_now
```

```python
import jax
import jax.numpy as jnp
from jax import lax
from jax.experimental import pallas as pl
from jax.experimental.pallas import tpu as pltpu
from jax.sharding import PartitionSpec as P

AXES = ("ma", "freq")
LANES = 128
VMEM_LIMIT = 12 * 1024 * 1024


def column(row):
    size = row.shape[1]
    spread = jnp.broadcast_to(row, (size, size))
    diagonal = lax.broadcasted_iota(jnp.int32, (size, size), 0) == lax.broadcasted_iota(
        jnp.int32, (size, size), 1
    )
    return jnp.sum(jnp.where(diagonal, spread, 0.0), axis=1, keepdims=True)


def stacked(real, imaginary):
    shape = (2, real.shape[1])
    first = lax.broadcasted_iota(jnp.int32, shape, 0) == 0
    return jnp.where(first, jnp.broadcast_to(real, shape), jnp.broadcast_to(imaginary, shape))


def beam_row(beam_ref, m, f, row, gain):
    real, imaginary = beam_ref[m, f, 0], beam_ref[m, f, 1]
    v_real, v_imag = row[0:1], row[1:2]
    p_real = jnp.sum(real * v_real + imaginary * v_imag, axis=1, keepdims=True) * gain
    p_imag = jnp.sum(real * v_imag - imaginary * v_real, axis=1, keepdims=True) * gain
    back_real = jnp.sum(real * p_real - imaginary * p_imag, axis=0, keepdims=True)
    back_imag = jnp.sum(real * p_imag + imaginary * p_real, axis=0, keepdims=True)
    return stacked(back_real, back_imag)


def counts(index, size, length):
    total = size * length
    out = []
    for f in range(length):
        channel = index * length + f
        out.append(
            jnp.where(channel > 0, 1.0, 0.0) + jnp.where(channel < total - 1, 1.0, 0.0)
        )
    return out


def local_rows(rows, m, beam_ref, noise_ref, inv, smooth, weights):
    out = []
    gains = noise_ref[m]
    for f, row in enumerate(rows):
        prior = weights[f] * row
        if f > 0:
            prior = prior - rows[f - 1]
        if f + 1 < len(rows):
            prior = prior - rows[f + 1]
        image = beam_row(beam_ref, m, f, row, column(gains[f : f + 1]))
        out.append(image + inv * row + smooth * prior)
    return out


def call(body, outs, *args):
    return pl.pallas_call(
        body,
        out_shape=outs,
        compiler_params=pltpu.CompilerParams(vmem_limit_bytes=VMEM_LIMIT),
    )(*args)


def shards(size, devices, right_side, start_field, beam, noise, inv_power, smooth):
    modes, length = right_side.shape[:2]
    width = right_side.shape[3]
    pair = size == 2
    field = jax.ShapeDtypeStruct(right_side.shape, jnp.float32)
    index = lax.axis_index("freq")
    inv_power = inv_power.reshape(1, width)
    smooth = smooth.reshape(1, width)
    up = [(i, i + 1) for i in range(size - 1)]
    down = [(j, i) for i, j in up]

    def exchanged(sends):
        if pair:
            return [lax.ppermute(sends[0], "freq", up + down)]
        return [lax.ppermute(sends[0], "freq", up), lax.ppermute(sends[1], "freq", down)]

    def edges(first, last, at):
        return [jnp.where(at == 0, last, first)] if pair else [last, first]

    def masks():
        at = lax.axis_index("freq")
        return at, jnp.where(at > 0, 1.0, 0.0), jnp.where(at < size - 1, 1.0, 0.0)

    def sides(values, below, above):
        low, high = (values[0], values[0]) if pair else (values[0], values[1])
        return low * below, high * above

    starts = exchanged(edges(start_field[:, 0], start_field[:, length - 1], index))

    def first(x_ref, b_ref, beam_ref, noise_ref, inv_ref, smooth_ref, p_ref):
        at, _, _ = masks()
        inv, strength = inv_ref[...], smooth_ref[...]
        weights = counts(at, size, length)

        def step(m, _):
            rows = [x_ref[m, f] for f in range(length)]
            images = local_rows(rows, m, beam_ref, noise_ref, inv, strength, weights)
            for f in range(length):
                p_ref[m, f] = b_ref[m, f] - images[f]
            return 0

        lax.fori_loop(0, modes, step, 0)

    partial = call(first, field, start_field, right_side, beam, noise, inv_power, smooth)

    ways = len(starts)
    send = jax.ShapeDtypeStruct((2, modes, 2, width), jnp.float32)

    def second(*refs):
        halo_refs, refs = refs[:ways], refs[ways:]
        p_ref, beam_ref, noise_ref, inv_ref, smooth_ref, r_ref, q_ref = refs[:7]
        send_refs = refs[7:]
        at, below, above = masks()
        inv, strength = inv_ref[...], smooth_ref[...]
        weights = counts(at, size, length)

        def step(m, _):
            low, high = sides([h[m] for h in halo_refs], below, above)
            rows = [p_ref[m, f] for f in range(length)]
            rows[0] = rows[0] + strength * low
            rows[-1] = rows[-1] + strength * high
            images = local_rows(rows, m, beam_ref, noise_ref, inv, strength, weights)
            for f in range(length):
                r_ref[m, f] = rows[f]
                q_ref[m, f] = images[f]
            for ref, r_edge, q_edge in zip(
                send_refs, edges(rows[0], rows[-1], at), edges(images[0], images[-1], at)
            ):
                ref[0, m] = r_edge
                ref[1, m] = q_edge
            return 0

        lax.fori_loop(0, modes, step, 0)

    resid, image, *sends = call(
        second, (field, field) + (send,) * ways, *starts, partial, beam, noise, inv_power, smooth
    )
    halos = exchanged(sends)

    def third(*refs):
        halo_refs, refs = refs[:ways], refs[ways:]
        r_ref, q_ref, beam_ref, noise_ref, inv_ref, smooth_ref, w_ref, z_ref, sums_ref = refs
        at, below, above = masks()
        inv, strength = inv_ref[...], smooth_ref[...]
        weights = counts(at, size, length)

        def step(m, sums):
            r_low, r_high = sides([h[0, m] for h in halo_refs], below, above)
            q_low, q_high = sides([h[1, m] for h in halo_refs], below, above)
            resids = [r_ref[m, f] for f in range(length)]
            rows = [q_ref[m, f] for f in range(length)]
            rows[0] = rows[0] - strength * r_low
            rows[-1] = rows[-1] - strength * r_high
            images = local_rows(rows, m, beam_ref, noise_ref, inv, strength, weights)
            images[0] = images[0] - strength * (q_low - below * strength * resids[0])
            images[-1] = images[-1] - strength * (q_high - above * strength * resids[-1])
            rr, rw, ww, wz = sums
            for f in range(length):
                w_ref[m, f] = rows[f]
                z_ref[m, f] = images[f]
                rr = rr + resids[f] * resids[f]
                rw = rw + resids[f] * rows[f]
                ww = ww + rows[f] * rows[f]
                wz = wz + rows[f] * images[f]
            return rr, rw, ww, wz

        zero = jnp.zeros((2, width), jnp.float32)
        sums = lax.fori_loop(0, modes, step, (zero, zero, zero, zero))
        lane = lax.broadcasted_iota(jnp.int32, (1, LANES), 1)
        packed = jnp.zeros((1, LANES), jnp.float32)
        for at_lane, value in enumerate(sums):
            packed = jnp.where(lane == at_lane, jnp.sum(value), packed)
        sums_ref[...] = jnp.broadcast_to(packed, (devices, LANES))

    along, twice, sums = call(
        third,
        (field, field, jax.ShapeDtypeStruct((devices, LANES), jnp.float32)),
        *halos, resid, image, beam, noise, inv_power, smooth,
    )
    sums = lax.all_to_all(sums, AXES, 0, 0, tiled=True)

    def last(sums_ref, x_ref, r_ref, w_ref, z_ref, out_ref, resid_ref):
        total = jnp.sum(sums_ref[...], axis=0, keepdims=True)
        lane = lax.broadcasted_iota(jnp.int32, (1, LANES), 1)
        rr, rw, ww, wz = [
            jnp.sum(jnp.where(lane == i, total, 0.0), axis=1, keepdims=True) for i in range(4)
        ]
        step0 = rr / rw
        cross = rw - step0 * ww
        rr1 = rr - 2.0 * step0 * rw + step0 * step0 * ww
        growth = rr1 / rr
        curve = rw - 2.0 * step0 * ww + step0 * step0 * wz + growth * cross
        step1 = rr1 / curve
        on_r = (step0 + step1 * (1.0 + growth)).reshape(1, 1, 1, 1)
        on_w = (step1 * step0).reshape(1, 1, 1, 1)
        r, w = r_ref[...], w_ref[...]
        out_ref[...] = x_ref[...] + on_r * r - on_w * w
        resid_ref[...] = r - on_r * w + on_w * z_ref[...]

    return tuple(call(last, (field, field), sums, start_field, resid, along, twice))


def solution(mesh):
    size, devices = mesh.shape["freq"], mesh.size

    def body(*args):
        return shards(size, devices, *args)

    in_specs = (
        P("ma", "freq", None, None),
        P("ma", "freq", None, None),
        P("ma", "freq", None, None, None),
        P("ma", "freq", None),
        P(),
        P(),
    )
    out_specs = (P("ma", "freq", None, None), P("ma", "freq", None, None))
    return jax.shard_map(body, mesh=mesh, in_specs=in_specs, out_specs=out_specs, check_vma=False)
```

```python
import jax
import jax.numpy as jnp
from jax import lax
from jax.experimental import pallas as pl
from jax.experimental.pallas import tpu as pltpu
from jax.sharding import PartitionSpec as P

AXES = ("ma", "freq")
LANES = 128
VMEM_LIMIT = 12 * 1024 * 1024


def column(row):
    size = row.shape[1]
    spread = jnp.broadcast_to(row, (size, size))
    diagonal = lax.broadcasted_iota(jnp.int32, (size, size), 0) == lax.broadcasted_iota(
        jnp.int32, (size, size), 1
    )
    return jnp.sum(jnp.where(diagonal, spread, 0.0), axis=1, keepdims=True)


def stacked(real, imaginary):
    shape = (2, real.shape[1])
    first = lax.broadcasted_iota(jnp.int32, shape, 0) == 0
    return jnp.where(first, jnp.broadcast_to(real, shape), jnp.broadcast_to(imaginary, shape))


def beam_row(beam_ref, m, f, row, gain):
    real, imaginary = beam_ref[m, f, 0], beam_ref[m, f, 1]
    v_real, v_imag = row[0:1], row[1:2]
    p_real = jnp.sum(real * v_real + imaginary * v_imag, axis=1, keepdims=True) * gain
    p_imag = jnp.sum(real * v_imag - imaginary * v_real, axis=1, keepdims=True) * gain
    back_real = jnp.sum(real * p_real - imaginary * p_imag, axis=0, keepdims=True)
    back_imag = jnp.sum(real * p_imag + imaginary * p_real, axis=0, keepdims=True)
    return stacked(back_real, back_imag)


def counts(index, size, length):
    total = size * length
    out = []
    for f in range(length):
        channel = index * length + f
        out.append(
            jnp.where(channel > 0, 1.0, 0.0) + jnp.where(channel < total - 1, 1.0, 0.0)
        )
    return out


def local_rows(rows, m, beam_ref, noise_ref, inv, smooth, weights):
    out = []
    gains = noise_ref[m]
    for f, row in enumerate(rows):
        prior = weights[f] * row
        if f > 0:
            prior = prior - rows[f - 1]
        if f + 1 < len(rows):
            prior = prior - rows[f + 1]
        image = beam_row(beam_ref, m, f, row, column(gains[f : f + 1]))
        out.append(image + inv * row + smooth * prior)
    return out


def call(body, outs, *args, **options):
    return pl.pallas_call(
        body,
        out_shape=outs,
        compiler_params=pltpu.CompilerParams(vmem_limit_bytes=VMEM_LIMIT),
        **options,
    )(*args)


def shards(size, devices, right_side, start_field, beam, noise, inv_power, smooth):
    modes, length = right_side.shape[:2]
    width = right_side.shape[3]
    assert length > 2
    pair = size == 2
    ways = 1 if pair else 2
    field = jax.ShapeDtypeStruct(right_side.shape, jnp.float32)
    edge = jax.ShapeDtypeStruct((modes, 2, width), jnp.float32)
    edge_pair = jax.ShapeDtypeStruct((2, modes, 2, width), jnp.float32)
    inv_power = inv_power.reshape(1, width)
    smooth = smooth.reshape(1, width)
    up = [(i, i + 1) for i in range(size - 1)]
    down = [(j, i) for i, j in up]

    def exchanged(sends):
        if pair:
            return [lax.ppermute(sends[0], "freq", up + down)]
        return [lax.ppermute(sends[1], "freq", up), lax.ppermute(sends[0], "freq", down)]

    def place():
        at = lax.axis_index("freq")
        below, above = at > 0, at < size - 1
        rows = [jnp.where(at == 0, length - 1, 0)] if pair else [0, length - 1]
        exists = [True] if pair else [below, above]
        return at, below, above, rows, exists

    def first(x_hbm, b_hbm, beam_hbm, noise_hbm, inv_hbm, smooth_hbm, p_ref, *refs):
        send_refs, refs = refs[:ways], refs[ways:]
        x_ref, b_ref, beam_ref, noise_ref, inv_ref, smooth_ref, few, many = refs
        small = [
            pltpu.make_async_copy(source, target, few.at[i])
            for i, (source, target) in enumerate(
                (
                    (x_hbm, x_ref),
                    (noise_hbm, noise_ref),
                    (inv_hbm, inv_ref),
                    (smooth_hbm, smooth_ref),
                    (b_hbm, b_ref),
                )
            )
        ]

        def large(m):
            return pltpu.make_async_copy(beam_hbm.at[m], beam_ref.at[m], many.at[m])

        for copy in small:
            copy.start()
        for m in range(modes):
            large(m).start()
        for copy in small:
            copy.wait()
        at, _, _, ends, _ = place()
        inv, strength = inv_ref[...], smooth_ref[...]
        weights = counts(at, size, length)

        def step(m, _):
            large(m).wait()
            rows = [x_ref[m, f] for f in range(length)]
            images = local_rows(rows, m, beam_ref, noise_ref, inv, strength, weights)
            for f in range(length):
                p_ref[m, f] = b_ref[m, f] - images[f]
            for ref, end in zip(send_refs, ends):
                ref[0, m] = x_ref[m, end]
                ref[1, m] = p_ref[m, end]
            return 0

        lax.fori_loop(0, modes, step, 0)

    loads = (start_field, right_side, beam, noise, inv_power, smooth)
    partial, *sends = call(
        first,
        (field,) + (edge_pair,) * ways,
        *[pltpu.with_memory_space_constraint(array, pltpu.HBM) for array in loads],
        in_specs=[pl.BlockSpec(memory_space=pltpu.HBM)] * len(loads),
        scratch_shapes=[pltpu.VMEM(array.shape, jnp.float32) for array in loads]
        + [pltpu.SemaphoreType.DMA((len(loads) - 1,)), pltpu.SemaphoreType.DMA((modes,))],
    )
    halos = exchanged(sends)

    def second(p_ref, beam_ref, noise_ref, inv_ref, smooth_ref, y_ref):
        at = lax.axis_index("freq")
        inv, strength = inv_ref[...], smooth_ref[...]
        weights = counts(at, size, length)

        def step(m, _):
            rows = [p_ref[m, f] for f in range(length)]
            images = local_rows(rows, m, beam_ref, noise_ref, inv, strength, weights)
            for f in range(length):
                y_ref[m, f] = images[f]
            return 0

        lax.fori_loop(0, modes, step, 0)

    image = call(second, field, partial, beam, noise, inv_power, smooth)

    def correct(*refs):
        halo_refs, send_refs, refs = refs[:ways], refs[ways : 2 * ways], refs[2 * ways :]
        p_ref, y_ref, beam_ref, noise_ref, inv_ref, smooth_ref = refs[:6]
        out_refs = refs[6:]
        at, _, _, ends, exists = place()
        inv, strength = inv_ref[...], smooth_ref[...]
        total = size * length

        def step(m, _):
            for halo, send, out, end, there in zip(halo_refs, send_refs, out_refs, ends, exists):
                channel = at * length + end
                weight = jnp.where(channel > 0, 1.0, 0.0) + jnp.where(channel < total - 1, 1.0, 0.0)
                added = strength * halo[0, m]
                theirs = halo[1, m] + strength * send[0, m]
                gain = column(noise_ref[m, pl.ds(end, 1), :])
                image = beam_row(beam_ref, m, end, added, gain)
                change = image + (inv + strength * weight) * added - strength * theirs
                out[m] = y_ref[m, end] + (change if there is True else jnp.where(there, change, 0.0))
            return 0

        lax.fori_loop(0, modes, step, 0)

    along_ends = call(
        correct, (edge,) * ways, *halos, *sends, partial, image, beam, noise, inv_power, smooth
    )
    far_ends = exchanged(along_ends)

    def third(*refs):
        halo_refs, end_refs, refs = refs[:ways], refs[ways : 2 * ways], refs[2 * ways :]
        p_ref, y_ref, beam_ref, noise_ref, inv_ref, smooth_ref = refs[:6]
        r_ref, w_ref, z_ref, sums_ref = refs[6:]
        at, below, above, _, _ = place()
        inv, strength = inv_ref[...], smooth_ref[...]
        weights = counts(at, size, length)

        def step(m, sums):
            added_low = jnp.where(below, strength * halo_refs[0][0, m], 0.0)
            added_high = jnp.where(above, strength * halo_refs[-1][0, m], 0.0)
            resids = [p_ref[m, f] for f in range(length)]
            resids[0] = resids[0] + added_low
            resids[-1] = resids[-1] + added_high
            rows = [y_ref[m, f] for f in range(length)]
            rows[0] = jnp.where(below, end_refs[0][m], rows[0])
            rows[-1] = jnp.where(above, end_refs[-1][m], rows[-1])
            rows[1] = rows[1] - strength * added_low
            rows[-2] = rows[-2] - strength * added_high
            images = local_rows(rows, m, beam_ref, noise_ref, inv, strength, weights)
            rr, rw, ww, wz = sums
            for f in range(length):
                r_ref[m, f] = resids[f]
                w_ref[m, f] = rows[f]
                z_ref[m, f] = images[f]
                rr = rr + resids[f] * resids[f]
                rw = rw + resids[f] * rows[f]
                ww = ww + rows[f] * rows[f]
                wz = wz + rows[f] * images[f]
            return rr, rw, ww, wz

        zero = jnp.zeros((2, width), jnp.float32)
        sums = lax.fori_loop(0, modes, step, (zero, zero, zero, zero))
        lane = lax.broadcasted_iota(jnp.int32, (1, LANES), 1)
        packed = jnp.zeros((1, LANES), jnp.float32)
        for at_lane, value in enumerate(sums):
            packed = jnp.where(lane == at_lane, jnp.sum(value), packed)
        sums_ref[...] = packed

    resid, along, twice, sums = call(
        third,
        (field, field, field, jax.ShapeDtypeStruct((1, LANES), jnp.float32)),
        *halos, *along_ends, partial, image, beam, noise, inv_power, smooth,
    )

    def cross(*refs):
        far_refs, end_refs, (sums_ref, smooth_ref, out_ref) = refs[:ways], refs[ways:-3], refs[-3:]
        _, _, _, _, exists = place()
        strength = smooth_ref[...]
        total = jnp.zeros((1, 1), jnp.float32)
        for far, end, there in zip(far_refs, end_refs, exists):
            product = jnp.sum(far[...] * end[...], axis=0)
            value = jnp.sum(strength * product, keepdims=True)
            total = total + (value if there is True else jnp.where(there, value, 0.0))
        lane = lax.broadcasted_iota(jnp.int32, (1, LANES), 1)
        packed = sums_ref[...] - jnp.where(lane == 3, total, 0.0)
        out_ref[...] = jnp.broadcast_to(packed, (devices, LANES))

    sums = call(
        cross, jax.ShapeDtypeStruct((devices, LANES), jnp.float32), *far_ends, *along_ends, sums, smooth
    )
    sums = lax.all_to_all(sums, AXES, 0, 0, tiled=True)

    def last(*refs):
        far_refs, refs = refs[:ways], refs[ways:]
        sums_ref, x_ref, r_ref, w_ref, z_ref, smooth_ref, out_ref, resid_ref = refs
        _, _, _, ends, exists = place()
        total = jnp.sum(sums_ref[...], axis=0, keepdims=True)
        lane = lax.broadcasted_iota(jnp.int32, (1, LANES), 1)
        rr, rw, ww, wz = [
            jnp.sum(jnp.where(lane == i, total, 0.0), axis=1, keepdims=True) for i in range(4)
        ]
        step0 = rr / rw
        crossed = rw - step0 * ww
        rr1 = rr - 2.0 * step0 * rw + step0 * step0 * ww
        growth = rr1 / rr
        curve = rw - 2.0 * step0 * ww + step0 * step0 * wz + growth * crossed
        step1 = rr1 / curve
        on_r = (step0 + step1 * (1.0 + growth)).reshape(1, 1, 1, 1)
        on_w = (step1 * step0).reshape(1, 1, 1, 1)
        r, w = r_ref[...], w_ref[...]
        out_ref[...] = x_ref[...] + on_r * r - on_w * w
        resid_ref[...] = r - on_r * w + on_w * z_ref[...]
        scale = (step1 * step0).reshape(1, 1, 1) * smooth_ref[...].reshape(1, 1, width)
        for far, end, there in zip(far_refs, ends, exists):
            value = scale * far[...]
            value = value if there is True else jnp.where(there, value, 0.0)
            resid_ref[:, end] = resid_ref[:, end] - value

    return tuple(
        call(last, (field, field), *far_ends, sums, start_field, resid, along, twice, smooth)
    )


def solution(mesh):
    size, devices = mesh.shape["freq"], mesh.size

    def body(*args):
        return shards(size, devices, *args)

    in_specs = (
        P("ma", "freq", None, None),
        P("ma", "freq", None, None),
        P("ma", "freq", None, None, None),
        P("ma", "freq", None),
        P(),
        P(),
    )
    out_specs = (P("ma", "freq", None, None), P("ma", "freq", None, None))
    return jax.shard_map(body, mesh=mesh, in_specs=in_specs, out_specs=out_specs, check_vma=False)
```

```python
import jax
import jax.numpy as jnp
from jax import lax
from jax.experimental import pallas as pl
from jax.experimental.pallas import tpu as pltpu
from jax.sharding import PartitionSpec as P

AXES = ("ma", "freq")
LANES = 128
VMEM_LIMIT = 12 * 1024 * 1024


def column(row):
    size = row.shape[1]
    spread = jnp.broadcast_to(row, (size, size))
    diagonal = lax.broadcasted_iota(jnp.int32, (size, size), 0) == lax.broadcasted_iota(
        jnp.int32, (size, size), 1
    )
    return jnp.sum(jnp.where(diagonal, spread, 0.0), axis=1, keepdims=True)


def stacked(real, imaginary):
    shape = (2, real.shape[1])
    first = lax.broadcasted_iota(jnp.int32, shape, 0) == 0
    return jnp.where(first, jnp.broadcast_to(real, shape), jnp.broadcast_to(imaginary, shape))


def beam_row(real, imaginary, row, gain):
    v_real, v_imag = row[0:1], row[1:2]
    p_real = jnp.sum(real * v_real + imaginary * v_imag, axis=1, keepdims=True) * gain
    p_imag = jnp.sum(real * v_imag - imaginary * v_real, axis=1, keepdims=True) * gain
    back_real = jnp.sum(real * p_real - imaginary * p_imag, axis=0, keepdims=True)
    back_imag = jnp.sum(real * p_imag + imaginary * p_real, axis=0, keepdims=True)
    return stacked(back_real, back_imag)


def call(body, outs, *args, **options):
    return pl.pallas_call(
        body,
        out_shape=outs,
        compiler_params=pltpu.CompilerParams(vmem_limit_bytes=VMEM_LIMIT),
        **options,
    )(*args)


def shards(size, devices, right_side, start_field, beam, noise, inv_power, smooth):
    modes, length, _, width = right_side.shape
    assert length > 2
    pair = size == 2
    ways = 1 if pair else 2
    ends = [0] if pair else [0, length - 1]
    inner = [j for j in range(length) if j not in ends]
    field = jax.ShapeDtypeStruct(right_side.shape, jnp.float32)
    edge = jax.ShapeDtypeStruct((modes, 2, width), jnp.float32)
    edge_pair = jax.ShapeDtypeStruct((2, modes, 2, width), jnp.float32)
    inv_power = inv_power.reshape(1, width)
    smooth = smooth.reshape(1, width)
    up = [(i, i + 1) for i in range(size - 1)]
    down = [(j, i) for i, j in up]

    def exchanged(sends):
        if pair:
            return [lax.ppermute(sends[0], "freq", up + down)]
        return [lax.ppermute(sends[1], "freq", up), lax.ppermute(sends[0], "freq", down)]

    def place():
        at = lax.axis_index("freq")
        if pair:
            order = [jnp.where(at == 0, length - 1 - j, j) for j in range(length)]
        else:
            order = list(range(length))
        weights = []
        for f in order:
            channel = at * length + f
            weights.append(
                jnp.where(channel > 0, 1.0, 0.0)
                + jnp.where(channel < size * length - 1, 1.0, 0.0)
            )
        exists = [True] if pair else [at > 0, at < size - 1]
        return order, weights, exists

    def kept(there, value):
        return value if there is True else jnp.where(there, value, 0.0)

    def operator(beam_of, noise_of, inv, strength, weights):
        def apply(rows, j):
            prior = weights[j] * rows[j]
            if j > 0:
                prior = prior - rows[j - 1]
            if j + 1 < length:
                prior = prior - rows[j + 1]
            real, imaginary = beam_of(j)
            image = beam_row(real, imaginary, rows[j], column(noise_of(j)))
            return image + inv * rows[j] + strength * prior

        return apply

    def whole(m, order, beam_ref, noise_ref, inv, strength, weights):
        return operator(
            lambda j: (beam_ref[m, order[j], 0], beam_ref[m, order[j], 1]),
            lambda j: noise_ref[m, pl.ds(order[j], 1), :],
            inv, strength, weights,
        )

    def first(x_hbm, b_hbm, beam_hbm, noise_hbm, inv_hbm, smooth_hbm, *refs):
        send_refs, refs = refs[:ways], refs[ways:]
        x_ref, b_ref, beam_ref, noise_ref, inv_ref, smooth_ref, sems = refs
        order, weights, _ = place()
        copies = [(beam_hbm.at[:, order[j]], beam_ref.at[k]) for k, j in enumerate(ends)]
        copies += [(b_hbm.at[:, order[j]], b_ref.at[k]) for k, j in enumerate(ends)]
        copies += [
            (x_hbm, x_ref), (noise_hbm, noise_ref), (inv_hbm, inv_ref), (smooth_hbm, smooth_ref)
        ]
        copies = [
            pltpu.make_async_copy(source, target, sems.at[i])
            for i, (source, target) in enumerate(copies)
        ]
        for copy in copies:
            copy.start()
        for copy in copies:
            copy.wait()
        inv, strength = inv_ref[...], smooth_ref[...]

        def step(m, _):
            rows = [x_ref[m, f] for f in order]
            for k, j in enumerate(ends):
                apply = operator(
                    lambda j, k=k: (beam_ref[k, m, 0], beam_ref[k, m, 1]),
                    lambda j: noise_ref[m, pl.ds(order[j], 1), :],
                    inv, strength, weights,
                )
                send_refs[k][0, m] = rows[j]
                send_refs[k][1, m] = b_ref[k, m] - apply(rows, j)
            return 0

        lax.fori_loop(0, modes, step, 0, unroll=True)

    loads = (start_field, right_side, beam, noise, inv_power, smooth)
    scratch = [
        start_field.shape,
        (ways, modes, 2, width),
        (ways, modes) + beam.shape[2:],
        noise.shape,
        (1, width),
        (1, width),
    ]
    sends = call(
        first,
        (edge_pair,) * ways,
        *[pltpu.with_memory_space_constraint(array, pltpu.HBM) for array in loads],
        in_specs=[pl.BlockSpec(memory_space=pltpu.HBM)] * len(loads),
        scratch_shapes=[pltpu.VMEM(shape, jnp.float32) for shape in scratch]
        + [pltpu.SemaphoreType.DMA((2 * ways + 4,))],
    )
    sends = list(sends)
    halos = exchanged(sends)

    def middle(x_ref, b_ref, beam_ref, noise_ref, inv_ref, smooth_ref, p_ref):
        order, weights, _ = place()
        inv, strength = inv_ref[...], smooth_ref[...]

        def step(m, _):
            apply = whole(m, order, beam_ref, noise_ref, inv, strength, weights)
            rows = [x_ref[m, f] for f in order]
            for j in inner:
                p_ref[m, j] = b_ref[m, order[j]] - apply(rows, j)
            return 0

        lax.fori_loop(0, modes, step, 0, unroll=2)

    partial = call(middle, field, start_field, right_side, beam, noise, inv_power, smooth)

    def second(*refs):
        halo_refs, send_refs, refs = refs[:ways], refs[ways : 2 * ways], refs[2 * ways :]
        p_ref, beam_ref, noise_ref, inv_ref, smooth_ref = refs[:5]
        r_refs, w_refs = refs[5 : 5 + ways], refs[5 + ways :]
        order, weights, exists = place()
        inv, strength = inv_ref[...], smooth_ref[...]

        def step(m, _):
            apply = whole(m, order, beam_ref, noise_ref, inv, strength, weights)
            rows = [None if j in ends else p_ref[m, j] for j in range(length)]
            for k, j in enumerate(ends):
                rows[j] = send_refs[k][1, m] + kept(exists[k], strength * halo_refs[k][0, m])
            for k, j in enumerate(ends):
                theirs = halo_refs[k][1, m] + strength * send_refs[k][0, m]
                r_refs[k][m] = rows[j]
                w_refs[k][m] = apply(rows, j) - kept(exists[k], strength * theirs)
            return 0

        lax.fori_loop(0, modes, step, 0, unroll=True)

    edges = call(
        second, (edge,) * (2 * ways), *halos, *sends, partial, beam, noise, inv_power, smooth
    )
    resid_ends, along_ends = edges[:ways], edges[ways:]
    far_ends = exchanged(along_ends)

    def third(*refs):
        r_ends, w_ends, refs = refs[:ways], refs[ways : 2 * ways], refs[2 * ways :]
        p_ref, beam_ref, noise_ref, inv_ref, smooth_ref = refs[:5]
        r_ref, w_ref, z_ref, sums_ref = refs[5:]
        order, weights, _ = place()
        inv, strength = inv_ref[...], smooth_ref[...]

        def step(m, sums):
            apply = whole(m, order, beam_ref, noise_ref, inv, strength, weights)
            resids = [
                r_ends[ends.index(j)][m] if j in ends else p_ref[m, j] for j in range(length)
            ]
            rows = [
                w_ends[ends.index(j)][m] if j in ends else apply(resids, j) for j in range(length)
            ]
            rr, rw, ww, wz = sums
            for j in range(length):
                image = apply(rows, j)
                r_ref[m, order[j]] = resids[j]
                w_ref[m, order[j]] = rows[j]
                z_ref[m, order[j]] = image
                rr = rr + resids[j] * resids[j]
                rw = rw + resids[j] * rows[j]
                ww = ww + rows[j] * rows[j]
                wz = wz + rows[j] * image
            return rr, rw, ww, wz

        zero = jnp.zeros((2, width), jnp.float32)
        sums = lax.fori_loop(0, modes, step, (zero, zero, zero, zero), unroll=2)
        lane = lax.broadcasted_iota(jnp.int32, (1, LANES), 1)
        packed = jnp.zeros((1, LANES), jnp.float32)
        for at_lane, value in enumerate(sums):
            packed = jnp.where(lane == at_lane, jnp.sum(value), packed)
        sums_ref[...] = packed

    resid, along, twice, sums = call(
        third,
        (field, field, field, jax.ShapeDtypeStruct((1, LANES), jnp.float32)),
        *resid_ends, *along_ends, partial, beam, noise, inv_power, smooth,
    )

    def cross(*refs):
        far_refs, end_refs, (sums_ref, smooth_ref, out_ref) = refs[:ways], refs[ways:-3], refs[-3:]
        _, _, exists = place()
        strength = smooth_ref[...]
        total = jnp.zeros((1, 1), jnp.float32)
        for far, end, there in zip(far_refs, end_refs, exists):
            product = jnp.sum(far[...] * end[...], axis=0)
            value = jnp.sum(strength * product, keepdims=True)
            total = total + kept(there, value)
        lane = lax.broadcasted_iota(jnp.int32, (1, LANES), 1)
        packed = sums_ref[...] - jnp.where(lane == 3, total, 0.0)
        out_ref[...] = jnp.broadcast_to(packed, (devices, LANES))

    sums = call(
        cross, jax.ShapeDtypeStruct((devices, LANES), jnp.float32), *far_ends, *along_ends, sums, smooth
    )
    sums = lax.all_to_all(sums, AXES, 0, 0, tiled=True)

    def last(*refs):
        far_refs, refs = refs[:ways], refs[ways:]
        sums_ref, x_ref, r_ref, w_ref, z_ref, smooth_ref, out_ref, resid_ref = refs
        order, _, exists = place()
        total = jnp.sum(sums_ref[...], axis=0, keepdims=True)
        lane = lax.broadcasted_iota(jnp.int32, (1, LANES), 1)
        rr, rw, ww, wz = [
            jnp.sum(jnp.where(lane == i, total, 0.0), axis=1, keepdims=True) for i in range(4)
        ]
        step0 = rr / rw
        crossed = rw - step0 * ww
        rr1 = rr - 2.0 * step0 * rw + step0 * step0 * ww
        growth = rr1 / rr
        curve = rw - 2.0 * step0 * ww + step0 * step0 * wz + growth * crossed
        step1 = rr1 / curve
        on_r = (step0 + step1 * (1.0 + growth)).reshape(1, 1, 1, 1)
        on_w = (step1 * step0).reshape(1, 1, 1, 1)
        r, w = r_ref[...], w_ref[...]
        out_ref[...] = x_ref[...] + on_r * r - on_w * w
        resid_ref[...] = r - on_r * w + on_w * z_ref[...]
        scale = (step1 * step0).reshape(1, 1, 1) * smooth_ref[...].reshape(1, 1, width)
        for far, j, there in zip(far_refs, ends, exists):
            value = kept(there, scale * far[...])
            resid_ref[:, order[j]] = resid_ref[:, order[j]] - value

    return tuple(
        call(last, (field, field), *far_ends, sums, start_field, resid, along, twice, smooth)
    )


def solution(mesh):
    size, devices = mesh.shape["freq"], mesh.size

    def body(*args):
        return shards(size, devices, *args)

    in_specs = (
        P("ma", "freq", None, None),
        P("ma", "freq", None, None),
        P("ma", "freq", None, None, None),
        P("ma", "freq", None),
        P(),
        P(),
    )
    out_specs = (P("ma", "freq", None, None), P("ma", "freq", None, None))
    return jax.shard_map(body, mesh=mesh, in_specs=in_specs, out_specs=out_specs, check_vma=False)
```

```python
import jax
import jax.numpy as jnp
from jax import lax
from jax.experimental import pallas as pl
from jax.experimental.pallas import tpu as pltpu
from jax.sharding import PartitionSpec as P

AXES = ("ma", "freq")
LANES = 128
VMEM_LIMIT = 12 * 1024 * 1024


def column(row):
    size = row.shape[1]
    spread = jnp.broadcast_to(row, (size, size))
    diagonal = lax.broadcasted_iota(jnp.int32, (size, size), 0) == lax.broadcasted_iota(
        jnp.int32, (size, size), 1
    )
    return jnp.sum(jnp.where(diagonal, spread, 0.0), axis=1, keepdims=True)


def stacked(real, imaginary):
    shape = (2, real.shape[1])
    first = lax.broadcasted_iota(jnp.int32, shape, 0) == 0
    return jnp.where(first, jnp.broadcast_to(real, shape), jnp.broadcast_to(imaginary, shape))


def beam_row(real, imaginary, row, gain):
    v_real, v_imag = row[0:1], row[1:2]
    p_real = jnp.sum(real * v_real + imaginary * v_imag, axis=1, keepdims=True) * gain
    p_imag = jnp.sum(real * v_imag - imaginary * v_real, axis=1, keepdims=True) * gain
    back_real = jnp.sum(real * p_real - imaginary * p_imag, axis=0, keepdims=True)
    back_imag = jnp.sum(real * p_imag + imaginary * p_real, axis=0, keepdims=True)
    return stacked(back_real, back_imag)


def call(body, outs, *args, **options):
    return pl.pallas_call(
        body,
        out_shape=outs,
        compiler_params=pltpu.CompilerParams(vmem_limit_bytes=VMEM_LIMIT),
        **options,
    )(*args)


def shards(size, devices, right_side, start_field, beam, noise, inv_power, smooth):
    modes, length, _, width = right_side.shape
    assert length > 2
    pair = size == 2
    ways = 1 if pair else 2
    ends = [0] if pair else [0, length - 1]
    inner = [j for j in range(length) if j not in ends]
    half = modes // 2
    parts = [(0, half), (half, modes)] if half else [(0, modes)]
    field = jax.ShapeDtypeStruct(right_side.shape, jnp.float32)
    edge = jax.ShapeDtypeStruct((modes, 2, width), jnp.float32)
    edge_pair = jax.ShapeDtypeStruct((2, modes, 2, width), jnp.float32)
    inv_power = inv_power.reshape(1, width)
    smooth = smooth.reshape(1, width)
    up = [(i, i + 1) for i in range(size - 1)]
    down = [(j, i) for i, j in up]

    def exchanged(sends):
        if pair:
            return [lax.ppermute(sends[0], "freq", up + down)]
        return [lax.ppermute(sends[1], "freq", up), lax.ppermute(sends[0], "freq", down)]

    def place():
        at = lax.axis_index("freq")
        if pair:
            order = [jnp.where(at == 0, length - 1 - j, j) for j in range(length)]
        else:
            order = list(range(length))
        weights = []
        for f in order:
            channel = at * length + f
            weights.append(
                jnp.where(channel > 0, 1.0, 0.0)
                + jnp.where(channel < size * length - 1, 1.0, 0.0)
            )
        exists = [True] if pair else [at > 0, at < size - 1]
        return order, weights, exists

    def kept(there, value):
        return value if there is True else jnp.where(there, value, 0.0)

    def operator(beam_of, noise_of, inv, strength, weights):
        def apply(rows, j):
            prior = weights[j] * rows[j]
            if j > 0:
                prior = prior - rows[j - 1]
            if j + 1 < length:
                prior = prior - rows[j + 1]
            real, imaginary = beam_of(j)
            image = beam_row(real, imaginary, rows[j], column(noise_of(j)))
            return image + inv * rows[j] + strength * prior

        return apply

    def whole(m, order, beam_ref, noise_ref, inv, strength, weights):
        return operator(
            lambda j: (beam_ref[m, order[j], 0], beam_ref[m, order[j], 1]),
            lambda j: noise_ref[m, pl.ds(order[j], 1), :],
            inv, strength, weights,
        )

    def first(x_hbm, b_hbm, beam_hbm, noise_hbm, inv_hbm, smooth_hbm, *refs):
        send_refs, refs = refs[:ways], refs[ways:]
        x_ref, b_ref, beam_ref, noise_ref, inv_ref, smooth_ref, sems = refs
        order, weights, _ = place()
        copies = [
            (x_hbm, x_ref), (noise_hbm, noise_ref), (inv_hbm, inv_ref), (smooth_hbm, smooth_ref)
        ]
        copies += [(b_hbm.at[:, order[j]], b_ref.at[k]) for k, j in enumerate(ends)]
        copies += [
            (beam_hbm.at[low:high, order[j]], beam_ref.at[k, low:high])
            for low, high in parts
            for k, j in enumerate(ends)
        ]
        copies = [
            pltpu.make_async_copy(source, target, sems.at[i])
            for i, (source, target) in enumerate(copies)
        ]
        for copy in copies:
            copy.start()
        for copy in copies[: 4 + ways]:
            copy.wait()
        inv, strength = inv_ref[...], smooth_ref[...]

        def step(m, _):
            rows = [x_ref[m, f] for f in order]
            for k, j in enumerate(ends):
                apply = operator(
                    lambda j, k=k: (beam_ref[k, m, 0], beam_ref[k, m, 1]),
                    lambda j: noise_ref[m, pl.ds(order[j], 1), :],
                    inv, strength, weights,
                )
                send_refs[k][0, m] = rows[j]
                send_refs[k][1, m] = b_ref[k, m] - apply(rows, j)
            return 0

        for i, (low, high) in enumerate(parts):
            for copy in copies[4 + ways * (i + 1) : 4 + ways * (i + 2)]:
                copy.wait()
            lax.fori_loop(low, high, step, 0, unroll=True)

    beam_hbm = pltpu.with_memory_space_constraint(beam, pltpu.HBM)
    loads = (start_field, right_side, beam, noise, inv_power, smooth)
    scratch = [
        start_field.shape,
        (ways, modes, 2, width),
        (ways, modes) + beam.shape[2:],
        noise.shape,
        (1, width),
        (1, width),
    ]
    sends = call(
        first,
        (edge_pair,) * ways,
        *[pltpu.with_memory_space_constraint(array, pltpu.HBM) for array in loads],
        in_specs=[pl.BlockSpec(memory_space=pltpu.HBM)] * len(loads),
        scratch_shapes=[pltpu.VMEM(shape, jnp.float32) for shape in scratch]
        + [pltpu.SemaphoreType.DMA((4 + ways * (1 + len(parts)),))],
    )
    sends = list(sends)
    halos = exchanged(sends)

    def middle(x_ref, b_ref, beam_hbm, noise_ref, inv_ref, smooth_ref, p_ref, beam_ref, sems):
        copies = [
            pltpu.make_async_copy(beam_hbm.at[low:high], beam_ref.at[low:high], sems.at[i])
            for i, (low, high) in enumerate(parts)
        ]
        for copy in copies:
            copy.start()
        order, weights, _ = place()
        inv, strength = inv_ref[...], smooth_ref[...]

        def step(m, _):
            apply = whole(m, order, beam_ref, noise_ref, inv, strength, weights)
            rows = [x_ref[m, f] for f in order]
            for j in inner:
                p_ref[m, j] = b_ref[m, order[j]] - apply(rows, j)
            return 0

        for copy, (low, high) in zip(copies, parts):
            copy.wait()
            lax.fori_loop(low, high, step, 0, unroll=2)

    in_vmem = pl.BlockSpec(memory_space=pltpu.VMEM)
    partial, beam = call(
        middle,
        (field, jax.ShapeDtypeStruct(beam.shape, jnp.float32)),
        start_field, right_side, beam_hbm, noise, inv_power, smooth,
        in_specs=[in_vmem] * 2 + [pl.BlockSpec(memory_space=pltpu.HBM)] + [in_vmem] * 3,
        scratch_shapes=[pltpu.SemaphoreType.DMA((len(parts),))],
    )

    def second(*refs):
        halo_refs, send_refs, refs = refs[:ways], refs[ways : 2 * ways], refs[2 * ways :]
        p_ref, beam_ref, noise_ref, inv_ref, smooth_ref = refs[:5]
        r_refs, w_refs = refs[5 : 5 + ways], refs[5 + ways :]
        order, weights, exists = place()
        inv, strength = inv_ref[...], smooth_ref[...]

        def step(m, _):
            apply = whole(m, order, beam_ref, noise_ref, inv, strength, weights)
            rows = [None if j in ends else p_ref[m, j] for j in range(length)]
            for k, j in enumerate(ends):
                rows[j] = send_refs[k][1, m] + kept(exists[k], strength * halo_refs[k][0, m])
            for k, j in enumerate(ends):
                theirs = halo_refs[k][1, m] + strength * send_refs[k][0, m]
                r_refs[k][m] = rows[j]
                w_refs[k][m] = apply(rows, j) - kept(exists[k], strength * theirs)
            return 0

        lax.fori_loop(0, modes, step, 0, unroll=True)

    edges = call(
        second, (edge,) * (2 * ways), *halos, *sends, partial, beam, noise, inv_power, smooth
    )
    resid_ends, along_ends = edges[:ways], edges[ways:]
    far_ends = exchanged(along_ends)

    def third(*refs):
        r_ends, w_ends, refs = refs[:ways], refs[ways : 2 * ways], refs[2 * ways :]
        p_ref, beam_ref, noise_ref, inv_ref, smooth_ref = refs[:5]
        r_ref, w_ref, z_ref, sums_ref = refs[5:]
        order, weights, _ = place()
        inv, strength = inv_ref[...], smooth_ref[...]

        def step(m, sums):
            apply = whole(m, order, beam_ref, noise_ref, inv, strength, weights)
            resids = [
                r_ends[ends.index(j)][m] if j in ends else p_ref[m, j] for j in range(length)
            ]
            rows = [
                w_ends[ends.index(j)][m] if j in ends else apply(resids, j) for j in range(length)
            ]
            rr, rw, ww, wz = sums
            for j in range(length):
                image = apply(rows, j)
                r_ref[m, order[j]] = resids[j]
                w_ref[m, order[j]] = rows[j]
                z_ref[m, order[j]] = image
                rr = rr + resids[j] * resids[j]
                rw = rw + resids[j] * rows[j]
                ww = ww + rows[j] * rows[j]
                wz = wz + rows[j] * image
            return rr, rw, ww, wz

        zero = jnp.zeros((2, width), jnp.float32)
        sums = lax.fori_loop(0, modes, step, (zero, zero, zero, zero), unroll=2)
        lane = lax.broadcasted_iota(jnp.int32, (1, LANES), 1)
        packed = jnp.zeros((1, LANES), jnp.float32)
        for at_lane, value in enumerate(sums):
            packed = jnp.where(lane == at_lane, jnp.sum(value), packed)
        sums_ref[...] = packed

    resid, along, twice, sums = call(
        third,
        (field, field, field, jax.ShapeDtypeStruct((1, LANES), jnp.float32)),
        *resid_ends, *along_ends, partial, beam, noise, inv_power, smooth,
    )

    def cross(*refs):
        far_refs, end_refs, (sums_ref, smooth_ref, out_ref) = refs[:ways], refs[ways:-3], refs[-3:]
        _, _, exists = place()
        strength = smooth_ref[...]
        total = jnp.zeros((1, 1), jnp.float32)
        for far, end, there in zip(far_refs, end_refs, exists):
            product = jnp.sum(far[...] * end[...], axis=0)
            value = jnp.sum(strength * product, keepdims=True)
            total = total + kept(there, value)
        lane = lax.broadcasted_iota(jnp.int32, (1, LANES), 1)
        packed = sums_ref[...] - jnp.where(lane == 3, total, 0.0)
        out_ref[...] = jnp.broadcast_to(packed, (devices, LANES))

    sums = call(
        cross, jax.ShapeDtypeStruct((devices, LANES), jnp.float32), *far_ends, *along_ends, sums, smooth
    )
    sums = lax.all_to_all(sums, AXES, 0, 0, tiled=True)

    def last(*refs):
        far_refs, refs = refs[:ways], refs[ways:]
        sums_ref, x_ref, r_ref, w_ref, z_ref, smooth_ref = refs[:6]
        out_hbm, resid_hbm, out_ref, resid_ref, sems = refs[6:]
        order, _, exists = place()
        total = jnp.sum(sums_ref[...], axis=0, keepdims=True)
        lane = lax.broadcasted_iota(jnp.int32, (1, LANES), 1)
        rr, rw, ww, wz = [
            jnp.sum(jnp.where(lane == i, total, 0.0), axis=1, keepdims=True) for i in range(4)
        ]
        step0 = rr / rw
        crossed = rw - step0 * ww
        rr1 = rr - 2.0 * step0 * rw + step0 * step0 * ww
        growth = rr1 / rr
        curve = rw - 2.0 * step0 * ww + step0 * step0 * wz + growth * crossed
        step1 = rr1 / curve
        on_r = (step0 + step1 * (1.0 + growth)).reshape(1, 1, 1, 1)
        on_w = (step1 * step0).reshape(1, 1, 1, 1)
        r, w = r_ref[...], w_ref[...]
        out_ref[...] = x_ref[...] + on_r * r - on_w * w
        out_copy = pltpu.make_async_copy(out_ref, out_hbm, sems.at[0])
        out_copy.start()
        resid_ref[...] = r - on_r * w + on_w * z_ref[...]
        scale = (step1 * step0).reshape(1, 1, 1) * smooth_ref[...].reshape(1, 1, width)
        for far, j, there in zip(far_refs, ends, exists):
            value = kept(there, scale * far[...])
            resid_ref[:, order[j]] = resid_ref[:, order[j]] - value
        resid_copy = pltpu.make_async_copy(resid_ref, resid_hbm, sems.at[1])
        resid_copy.start()
        out_copy.wait()
        resid_copy.wait()

    return tuple(
        call(
            last,
            (field, field),
            *far_ends, sums, start_field, resid, along, twice, smooth,
            out_specs=(pl.BlockSpec(memory_space=pltpu.HBM),) * 2,
            scratch_shapes=[pltpu.VMEM(field.shape, jnp.float32)] * 2
            + [pltpu.SemaphoreType.DMA((2,))],
        )
    )


def solution(mesh):
    size, devices = mesh.shape["freq"], mesh.size

    def body(*args):
        return shards(size, devices, *args)

    in_specs = (
        P("ma", "freq", None, None),
        P("ma", "freq", None, None),
        P("ma", "freq", None, None, None),
        P("ma", "freq", None),
        P(),
        P(),
    )
    out_specs = (P("ma", "freq", None, None), P("ma", "freq", None, None))
    return jax.shard_map(body, mesh=mesh, in_specs=in_specs, out_specs=out_specs, check_vma=False)
```
